32 devices in a mesh: freq: 2 (over x), leaf: 16 (over z, y, core).
Axes of the slice: x: 2, y: 2, z: 4, core: 2. Of those that a mesh axis runs over, the one named last changes fastest.
Arguments:
- rhs: float32 [128, 256, 128], P(('freq', 'leaf')), parts along dimension 0, may hold values from -6 to 6
- leaf_q: float32 [128, 256, 256], P(('freq', 'leaf')), parts along dimension 0, may hold values from -0.375 to 0.375
- leaf_e: float32 [128, 256, 256], P(('freq', 'leaf')), parts along dimension 0, may hold values from -0.375 to 0.375
- leaf_w: float32 [128, 256, 128], P(('freq', 'leaf')), parts along dimension 0, may hold values from -0.375 to 0.375
- node_q: float32 [96, 256, 256], P(('freq', 'leaf')), parts along dimension 0, may hold values from -0.375 to 0.375
- node_e: float32 [96, 256, 256], P(('freq', 'leaf')), parts along dimension 0, may hold values from -0.375 to 0.375
- node_w: float32 [96, 256, 128], P(('freq', 'leaf')), parts along dimension 0, may hold values from -0.375 to 0.375
- top_q: float32 [128, 256, 256], P(('freq', 'leaf')), parts along dimension 0, as said below
- top_e: float32 [128, 256, 256], P(('freq', 'leaf')), parts along dimension 0, as said below
- top_w: float32 [128, 256, 128], P(('freq', 'leaf')), parts along dimension 0, as said below
Outputs:
- solution: float32 [128, 256, 128], P(('freq', 'leaf')), parts along dimension 0
The draws below stay inside these ranges and needn't reach their ends.
There are 2 independent parts, one for each index of `freq`. The reference program is written for one: setup_inputs(seed, part) draws one part's arguments, and reference() takes and returns one part's arrays. A program takes and returns all parts, laid end to end along the dimension named above; each array names one. Nothing has to cross between parts.
Inputs may be any that keep to these rules, and one draw needn't show every extreme that they name: Device d's 4 rows of top_q hold, in row l-1, the transform of the level l node d // 2^l; devices with equal d // 2^l hold equal rows l-1. `top_e`: likewise for the inverted blocks: row l-1 of device d belongs to node d // 2^l of level l and is equal on all devices of that node. `top_w`: likewise for the generators: row l-1 of device d belongs to node d // 2^l of level l and is equal on all devices of that node.
All inputs are finite; a program needn't handle non-finite values.
Results may differ from the reference program's by a relative error of at most 0.00012.
Values sent between devices are 32-bit elements; how exact they have to be, the bound alone decides.
A program may use at most 64 MiB of HBM per device.

```python
import jax
import jax.numpy as jnp
from jax import lax

M = 256
K = 128
R = 128
LEAF_DEV = 4
UPPER = 4
LEAVES = 64
N_LEAF = 16


def ancestors(key, salt, columns):
    blocks = []
    for level in range(1, UPPER + 1):
        count = N_LEAF // 2 ** level
        drawn = jax.random.normal(jax.random.fold_in(key, salt + level), (count, M, columns), jnp.float32) * M ** (-0.5)
        blocks.append(jnp.repeat(drawn, 2 ** level, axis=0))
    return jnp.stack(blocks, axis=1).reshape(N_LEAF * UPPER, M, columns)


def draw_top_q(key, part):
    return ancestors(key, 1000, M)


def draw_top_e(key, part):
    return ancestors(key, 2000, M)


def draw_top_w(key, part):
    return ancestors(key, 3000, K)


def levels(stream_key, extent, cuts, low, top_value):
    factor_of = 1.0
    for dim, parts in cuts:
        steps = jax.random.uniform(jax.random.fold_in(jax.random.fold_in(stream_key, 6), dim), (parts,), jnp.float32, low / len(cuts), top_value / len(cuts))
        factor_of = factor_of * jnp.repeat(jnp.exp(steps), extent[dim] // parts).reshape((-1,) + (1,) * (len(extent) - 1 - dim))
    return factor_of


def bell_draw(stream_key, shape, scale, limit, shards=(), kind=jnp.bfloat16):
    values = scale * jax.random.normal(stream_key, shape, jnp.float32)
    if shards:
        values = values * levels(stream_key, shape, shards, -0.22, 0.18)
    return jnp.clip(values, -limit, limit).astype(kind)


def setup_inputs(seed: int = 0, part: int = 0) -> dict:
    seeds = jax.random.split(jax.random.key(seed), 11)
    part_splits = jax.random.split(jax.random.fold_in(seeds[10], part), 11)
    rhs = bell_draw(part_splits[0], (LEAVES, M, R), 1.0, 6.0, ((0, 16),), jnp.float32)
    leaf_q = bell_draw(part_splits[1], (LEAVES, M, M), M ** -0.5, 0.375, ((0, 16),), jnp.float32)
    leaf_e = bell_draw(part_splits[2], (LEAVES, M, M), M ** -0.5, 0.375, ((0, 16),), jnp.float32)
    leaf_w = bell_draw(part_splits[3], (LEAVES, M, K), M ** -0.5, 0.375, ((0, 16),), jnp.float32)
    node_q = bell_draw(part_splits[4], (N_LEAF * (LEAF_DEV - 1), M, M), M ** -0.5, 0.375, ((0, 16),), jnp.float32)
    node_e = bell_draw(part_splits[5], (N_LEAF * (LEAF_DEV - 1), M, M), M ** -0.5, 0.375, ((0, 16),), jnp.float32)
    node_w = bell_draw(part_splits[6], (N_LEAF * (LEAF_DEV - 1), M, K), M ** -0.5, 0.375, ((0, 16),), jnp.float32)
    top_q = draw_top_q(jax.random.fold_in(jax.random.fold_in(seeds[10], part), 71), part)
    top_e = draw_top_e(jax.random.fold_in(jax.random.fold_in(seeds[10], part), 71), part)
    top_w = draw_top_w(jax.random.fold_in(jax.random.fold_in(seeds[10], part), 71), part)
    return dict(rhs=rhs, leaf_q=leaf_q, leaf_e=leaf_e, leaf_w=leaf_w, node_q=node_q, node_e=node_e, node_w=node_w, top_q=top_q, top_e=top_e, top_w=top_w)


HIGH = lax.Precision.HIGHEST


def batched(mats, vecs):
    return jnp.einsum("nij,njr->nir", mats, vecs, precision=HIGH)


def batched_t(mats, vecs):
    return jnp.einsum("nji,njr->nir", mats, vecs, precision=HIGH)


def upward(qmat, emat, wmat, vecs):
    values = batched(emat, batched(qmat, vecs))
    return values, batched_t(wmat, values)


def downward(qmat, emat, wmat, values, parent):
    return batched_t(qmat, values - batched(emat, batched(wmat, parent)))


def pick_level(gens, level):
    count = LEAF_DEV // 2 ** level
    offset = LEAF_DEV - 2 * count
    shaped = gens.reshape(N_LEAF, LEAF_DEV - 1, gens.shape[1], gens.shape[2])
    return shaped[:, offset:offset + count].reshape(-1, gens.shape[1], gens.shape[2])


def top_level(gens, level):
    shaped = gens.reshape(N_LEAF, UPPER, gens.shape[1], gens.shape[2])
    return shaped[::2 ** level, level - 1]


def reference(rhs, leaf_q, leaf_e, leaf_w, node_q, node_e, node_w, top_q, top_e, top_w):
    local_levels = LEAF_DEV.bit_length() - 1
    upper_levels = N_LEAF.bit_length() - 1
    width = leaf_w.shape[2]
    cols = rhs.shape[2]
    values, reduced = upward(leaf_q, leaf_e, leaf_w, rhs)
    local_values = [values]
    for level in range(1, local_levels + 1):
        stacked = reduced.reshape(-1, 2 * width, cols)
        values, reduced = upward(pick_level(node_q, level), pick_level(node_e, level), pick_level(node_w, level), stacked)
        local_values.append(values)
    upper_values = []
    for level in range(1, upper_levels + 1):
        stacked = reduced.reshape(-1, 2 * width, cols)
        values, reduced = upward(top_level(top_q, level), top_level(top_e, level), top_level(top_w, level), stacked)
        upper_values.append(values)
    answer = upper_values[-1]
    for level in range(upper_levels, 1, -1):
        parent = answer.reshape(-1, width, cols)
        answer = downward(top_level(top_q, level - 1), top_level(top_e, level - 1), top_level(top_w, level - 1), upper_values[level - 2], parent)
    parent = answer.reshape(-1, width, cols)
    for level in range(local_levels, 0, -1):
        answer = downward(pick_level(node_q, level), pick_level(node_e, level), pick_level(node_w, level), local_values[level], parent)
        parent = answer.reshape(-1, width, cols)
    return downward(leaf_q, leaf_e, leaf_w, local_values[0], parent)
```

```python
import functools

import jax
import jax.numpy as jnp
from jax import lax
from jax.experimental import pallas as pl
from jax.experimental.pallas import tpu as pltpu
from jax.sharding import PartitionSpec as P

MESH = pl.DeviceIdType.MESH
F32, BF16 = jnp.float32, jnp.bfloat16
NN, NT, TN = ((1,), (0,)), ((1,), (1,)), ((0,), (0,))


def split(x):
    hi = x.astype(BF16)
    return hi, (x - hi.astype(F32)).astype(BF16)


def dot3(a, b, dims=NN):
    def one(x, y):
        return lax.dot_general(x, y, (dims, ((), ())), preferred_element_type=F32)

    return one(a[0], b[0]) + (one(a[0], b[1]) + one(a[1], b[0]))


def cat(*xs):
    return jnp.concatenate(xs, axis=1)


def plan(n):
    total = n.bit_length() - 1
    cuts = [0]
    while cuts[-1] < total:
        cuts.append(min(cuts[-1] + 2, total))
    if len(cuts) == 2:
        cuts = [0, total - 1, total]
    return list(zip(cuts[:-1], cuts[1:]))


def kernel(n, *refs):
    (rhs_h, lq_h, le_h, lw_h, nq_h, ne_h, nw_h, tq_h, te_h, tw_h, out_h,
     rhs, lq, le, lw, nq, ne, nw, tq, te, tw, out,
     ye, ud, red, sent0, sent1, full, part, spread, sendg, gath,
     mat_hi, mat_lo, dn, fin_hi, fin_lo,
     sem_in, sem_out, send_sem, recv_sem, gsend_sem, grecv_sem) = refs
    stages = plan(n)
    levels = n.bit_length() - 1
    s = stages[0][1]
    S = 2**s
    leaves = rhs.shape[0]
    K = lw.shape[2]
    R = rhs.shape[2]
    r = R // S
    me = lax.axis_index("leaf")
    pos = lax.rem(me, S)

    def side(level):
        return lax.rem(me // 2 ** (level - 1), 2)

    loads = {}
    count = 0

    def load(name, src, dst, i):
        nonlocal count
        copy = pltpu.make_async_copy(src.at[i], dst.at[i], sem_in.at[count])
        copy.start()
        loads[name, i] = copy
        count += 1

    for i in range(leaves):
        load("rhs", rhs_h, rhs, i)
        load("lq", lq_h, lq, i)
        load("le", le_h, le, i)
        load("lw", lw_h, lw, i)
    for i in range(leaves - 1):
        load("nq", nq_h, nq, i)
        load("ne", ne_h, ne, i)
        load("nw", nw_h, nw, i)
    for i in range(levels):
        load("tq", tq_h, tq, i)
        load("te", te_h, te, i)
        load("tw", tw_h, tw, i)

    messages = []
    for a, b in stages:
        for d in range(1, 2 ** (b - a)):
            messages.append((a, d))

    barrier = pltpu.get_barrier_semaphore()
    for a, d in messages:
        pl.semaphore_signal(
            barrier, inc=1, device_id={"leaf": me ^ (d << a)}, device_id_type=MESH
        )

    nodes = [(lq, le, lw, i, ("lq", "le", "lw")) for i in range(leaves)]
    nodes += [(nq, ne, nw, i, ("nq", "ne", "nw")) for i in range(leaves - 1)]

    def up(k, vecs):
        q, e, w, i, names = nodes[k]
        loads[names[0], i].wait()
        t = dot3(split(q[i]), split(vecs))
        loads[names[1], i].wait()
        loads[names[2], i].wait()
        both = dot3(split(e[i]), split(cat(t, w[i])))
        ye[k] = both
        return split(both[:, :R]), split(w[i])

    def solve(k):
        q, _, _, i, _ = nodes[k]
        ud[k] = dot3(split(q[i]), split(ye[k]), TN)

    def top(level):
        i = level - 1
        for name in ("tq", "te", "tw"):
            loads[name, i].wait()
        right = side(level) == 1
        q, w = tq[i], tw[i]
        if level == levels:
            rows = jnp.where(right, te[i, K:, :], te[i, :K, :])
            m = dot3(split(rows), split(q))
            height = K
        else:
            mine = jnp.where(right, q[:, K:], q[:, :K])
            z = cat(w, mine)
            if level == s:
                z = cat(z, jnp.where(right, q[:, :K], q[:, K:]))
            height = z.shape[1]
            ze = dot3(split(z), split(te[i]), TN)
            zs = split(ze)
            m = dot3(zs, split(q))
            dn[i, : height - K] = dot3(split(ze[K:]), split(w))
        own = jnp.where(right, m[:, K:], m[:, :K])
        sib = jnp.where(right, m[:, :K], m[:, K:])
        mat_hi[i, 0, :height], mat_lo[i, 0, :height] = split(own)
        mat_hi[i, 1, :height], mat_lo[i, 1, :height] = split(sib)
        return height

    def mat(level, which, low, high):
        i = level - 1
        return mat_hi[i, which, low:high], mat_lo[i, which, low:high]

    for k in range(leaves):
        loads["rhs", k].wait()
        y, w = up(k, rhs[k])
        red[k // 2, k % 2 * K : k % 2 * K + K] = dot3(w, y, TN)
    below, k = leaves, leaves
    heights = {}
    base = 0
    while below > 1:
        if below == 2:
            heights[1] = top(1)
        nxt = below // 2
        for j in range(nxt):
            y, w = up(k, red[base + j])
            if nxt > 1:
                red[base + nxt + j // 2, j % 2 * K : j % 2 * K + K] = dot3(w, y, TN)
            else:
                reduced = dot3(y, w, TN)
            k += 1
        base += nxt
        below = nxt

    pl.semaphore_wait(barrier, len(messages))

    def exchange(index, a, d, src, dst):
        copy = pltpu.make_async_remote_copy(
            src_ref=src,
            dst_ref=dst,
            send_sem=send_sem.at[index],
            recv_sem=recv_sem.at[index],
            device_id={"leaf": me ^ (d << a)},
            device_id_type=MESH,
        )
        copy.start()
        return copy

    u_top = {}
    copies = {}
    index = 0
    current = reduced
    for number, (a, b) in enumerate(stages):
        first = number == 0
        moved = current
        for l in range(a, b):
            if l > a:
                moved = dot3(split(moved), mat(l, 0, 0, K), NT)
            if first:
                sent0[l] = moved.reshape(S, r, K)
            else:
                sent1[l] = moved
            for d in range(2 ** (l - a), 2 ** (l - a + 1)):
                if first and l + 1 < s:
                    copies[a, d] = exchange(index, a, d, sent0.at[l], full.at[d])
                elif first:
                    block = lax.rem(me ^ d, S)
                    copies[a, d] = exchange(index, a, d, sent0.at[l, block], part.at[index])
                else:
                    copies[a, d] = exchange(index, a, d, sent1.at[l], part.at[index])
                index += 1
        if first:
            for l in range(2, levels + 1):
                if l <= stages[1][1]:
                    heights[l] = top(l)
            for k in range(leaves):
                solve(k)
        if number == 1 or len(stages) == 1:
            for l in range(stages[1][1] + 1, levels + 1):
                heights[l] = top(l)
            for k in range(leaves, 2 * leaves - 1):
                solve(k)
            k = 2 * leaves - 2
            u, d_ = ud[k, :, :R], ud[k, :, R:]
            for l in range(1, s):
                ds = split(d_)
                u = u - dot3(ds, split(u_top[l]), NT)
                d_ = -dot3(ds, split(dn[l - 1, :K]))
            ud[k] = cat(u, d_)
            count_here, start = 1, k
            while count_here < leaves:
                kids = start - 2 * count_here
                for j in range(2 * count_here):
                    half = j % 2 * K
                    both = split(ud[start + j // 2, half : half + K])
                    kid = ud[kids + j]
                    moved_ = dot3(split(kid[:, R:]), both)
                    ud[kids + j] = cat(kid[:, :R] - moved_[:, :R], -moved_[:, R:])
                start, count_here = kids, 2 * count_here
            for j in range(leaves):
                fin_hi[j], fin_lo[j] = split(ud[j, :, R:])
        if b == levels:
            m = None
            for l in range(levels - 1, s - 1, -1):
                lower = dn[l - 1, : heights[l] - K]
                step = mat(levels, 1, 0, K) if m is None else split(m)
                m = -dot3(split(lower), step)
            last = split(m)
        for l in range(a + 1, b + 1):
            group = range(2 ** (l - a - 1), 2 ** (l - a))
            if l == s:
                spread[...] = current.reshape(S, r, K)
                current = spread[pos]
            known = None
            if l < levels:
                h = heights[l]
                known = dot3(split(current), mat(l, 0, 0, h), NT)
            else:
                known = dot3(split(current), mat(l, 0, 0, K), NT)
                for low in range(levels - 1, s - 1, -1):
                    lower = split(dn[low - 1, : heights[low] - K])
                    known = u_top[low] - dot3(split(known), lower, NT)
            sib = None
            for d in group:
                copies[a, d].wait_recv()
                if first and l < s:
                    got = full[d].reshape(R, K)
                else:
                    got = part[messages.index((a, d))]
                sib = got if sib is None else sib + got
            if l < levels:
                both = known + dot3(split(sib), mat(l, 1, 0, h), NT)
                current = both[:, :K]
                u_top[l] = both[:, K:]
            else:
                answer = known + dot3(split(sib), last, NT)

    sendg[0] = answer[:, :K]
    sendg[1] = answer[:, K:]
    gcopies = []
    for d in range(S - 1, 0, -1):
        copy = pltpu.make_async_remote_copy(
            src_ref=sendg.at[1 if d >= S // 2 else 0],
            dst_ref=gath.at[pos],
            send_sem=gsend_sem.at[d],
            recv_sem=grecv_sem.at[d],
            device_id={"leaf": me ^ d},
            device_id_type=MESH,
        )
        copy.start()
        gcopies.append(copy)
    gath[pos] = answer[:, :K]
    for copy in gcopies:
        copy.wait_recv()
    g = split(gath[...].reshape(R, K))
    outs = []
    for j in range(leaves):
        out[j] = ud[j, :, :R] - dot3((fin_hi[j], fin_lo[j]), g, NT)
        copy = pltpu.make_async_copy(out.at[j], out_h.at[j], sem_out.at[j])
        copy.start()
        outs.append(copy)
    for copy in copies.values():
        copy.wait_send()
    for copy in gcopies:
        copy.wait_send()
    for copy in outs:
        copy.wait()


def body(n, *args):
    rhs, leaf_w, top_q = args[0], args[3], args[7]
    leaves, M, R = rhs.shape
    K = leaf_w.shape[2]
    levels = n.bit_length() - 1
    stages = plan(n)
    s = stages[0][1]
    S = 2**s
    r = R // S
    msgs = sum(2 ** (b - a) - 1 for a, b in stages)
    local = 2 * leaves - 1
    scratch = [pltpu.VMEM(x.shape, x.dtype) for x in args]
    scratch += [
        pltpu.VMEM((leaves, M, R), F32),
        pltpu.VMEM((local, M, R + K), F32),
        pltpu.VMEM((local, M, R + K), F32),
        pltpu.VMEM((leaves, 2 * K, R), F32),
        pltpu.VMEM((s, S, r, K), F32),
        pltpu.VMEM((levels, r, K), F32),
        pltpu.VMEM((S, S, r, K), F32),
        pltpu.VMEM((msgs, r, K), F32),
        pltpu.VMEM((S, r, K), F32),
        pltpu.VMEM((2, r, K), F32),
        pltpu.VMEM((S, r, K), F32),
        pltpu.VMEM((levels, 2, 3 * K, K), BF16),
        pltpu.VMEM((levels, 2, 3 * K, K), BF16),
        pltpu.VMEM((levels, 2 * K, K), F32),
        pltpu.VMEM((leaves, M, K), BF16),
        pltpu.VMEM((leaves, M, K), BF16),
        pltpu.SemaphoreType.DMA((4 * leaves + 3 * (leaves - 1) + 3 * levels,)),
        pltpu.SemaphoreType.DMA((leaves,)),
        pltpu.SemaphoreType.DMA((msgs,)),
        pltpu.SemaphoreType.DMA((msgs,)),
        pltpu.SemaphoreType.DMA((S,)),
        pltpu.SemaphoreType.DMA((S,)),
    ]
    return pl.pallas_call(
        functools.partial(kernel, n),
        out_shape=jax.ShapeDtypeStruct((leaves, M, R), F32),
        in_specs=[pl.BlockSpec(memory_space=pl.ANY)] * len(args),
        out_specs=pl.BlockSpec(memory_space=pl.ANY),
        scratch_shapes=scratch,
        compiler_params=pltpu.CompilerParams(collective_id=0, has_side_effects=True),
    )(*args)


def solution(mesh):
    spec = P(("freq", "leaf"), None, None)
    return jax.shard_map(
        functools.partial(body, mesh.shape["leaf"]),
        mesh=mesh,
        in_specs=(spec,) * 10,
        out_specs=spec,
        check_vma=False,
    )
```

```python
import functools

import jax
import jax.numpy as jnp
from jax import lax
from jax.experimental import pallas as pl
from jax.experimental.pallas import tpu as pltpu
from jax.sharding import PartitionSpec as P

MESH = pl.DeviceIdType.MESH
F32, BF16 = jnp.float32, jnp.bfloat16
NN, NT, TN = ((1,), (0,)), ((1,), (1,)), ((0,), (0,))


def split(x):
    hi = x.astype(BF16)
    return hi, (x - hi.astype(F32)).astype(BF16)


def dot3(a, b, dims=NN):
    def one(x, y):
        return lax.dot_general(x, y, (dims, ((), ())), preferred_element_type=F32)

    return one(a[0], b[0]) + (one(a[0], b[1]) + one(a[1], b[0]))


def cat(*xs):
    return jnp.concatenate(xs, axis=1)


def plan(n):
    total = n.bit_length() - 1
    cuts = [0]
    while cuts[-1] < total:
        cuts.append(min(cuts[-1] + 2, total))
    if len(cuts) == 2:
        cuts = [0, total - 1, total]
    return list(zip(cuts[:-1], cuts[1:]))


def kernel(n, *refs):
    (rhs_h, lq_h, le_h, lw_h, nq_h, ne_h, nw_h, tq_h, te_h, tw_h, out_h,
     rhs, lq, le, lw, nq, ne, nw, tq, te, tw, out,
     ye, ud, stacked, up_hi, up_lo, sent0, sent1, full, part, spread, sendg, gath,
     mat_hi, mat_lo, dn, fin_hi, fin_lo,
     sem_in, sem_out, send_sem, recv_sem, gsend_sem, grecv_sem) = refs
    stages = plan(n)
    levels = n.bit_length() - 1
    s = stages[0][1]
    S = 2**s
    leaves = rhs.shape[0]
    K = lw.shape[2]
    R = rhs.shape[2]
    r = R // S
    me = lax.axis_index("leaf")
    pos = lax.rem(me, S)

    def side(level):
        return lax.rem(me // 2 ** (level - 1), 2)

    loads = {}
    count = 0

    def load(name, src, dst, i):
        nonlocal count
        copy = pltpu.make_async_copy(src.at[i], dst.at[i], sem_in.at[count])
        copy.start()
        loads[name, i] = copy
        count += 1

    for i in range(leaves - 1):
        load("nw", nw_h, nw, i)
        load("ne", ne_h, ne, i)
        load("nq", nq_h, nq, i)
    for i in range(leaves):
        load("rhs", rhs_h, rhs, i)
        load("lq", lq_h, lq, i)
    for i in range(leaves):
        load("lw", lw_h, lw, i)
        load("le", le_h, le, i)
    for i in range(levels):
        load("tq", tq_h, tq, i)
        load("te", te_h, te, i)
        load("tw", tw_h, tw, i)

    messages = []
    for a, b in stages:
        for d in range(1, 2 ** (b - a)):
            messages.append((a, d))

    barrier = pltpu.get_barrier_semaphore()
    for a, d in messages:
        pl.semaphore_signal(
            barrier, inc=1, device_id={"leaf": me ^ (d << a)}, device_id_type=MESH
        )

    def factors(k):
        return (lq, le, lw, k) if k < leaves else (nq, ne, nw, k - leaves)

    def values(k, t):
        _, e, w, i = factors(k)
        ye[k] = dot3(split(jnp.concatenate([t, w[i].T], axis=0)), split(e[i]), NT)

    def solve(k):
        q, _, _, i = factors(k)
        ud[k] = dot3(split(ye[k]), split(q[i]))

    def node(k):
        i = k - leaves
        values(k, dot3(split(stacked[i]), split(nq[i]), NT))
        solve(k)

    def top(level):
        i = level - 1
        for name in ("tq", "te", "tw"):
            loads[name, i].wait()
        right = side(level) == 1
        q, w = tq[i], tw[i]
        if level == levels:
            rows = jnp.where(right, te[i, K:, :], te[i, :K, :])
            m = dot3(split(rows), split(q))
            height = K
        else:
            mine = jnp.where(right, q[:, K:], q[:, :K])
            z = cat(w, mine)
            if level == s:
                z = cat(z, jnp.where(right, q[:, :K], q[:, K:]))
            height = z.shape[1]
            ze = dot3(split(z), split(te[i]), TN)
            zs = split(ze)
            m = dot3(zs, split(q))
            dn[i, : height - K] = dot3(split(ze[K:]), split(w))
        own = jnp.where(right, m[:, K:], m[:, :K])
        sib = jnp.where(right, m[:, :K], m[:, K:])
        mat_hi[i, 0, :height], mat_lo[i, 0, :height] = split(own)
        mat_hi[i, 1, :height], mat_lo[i, 1, :height] = split(sib)
        return height

    def mat(level, which, low, high):
        i = level - 1
        return mat_hi[i, which, low:high], mat_lo[i, which, low:high]

    for i in range(leaves - 1):
        for name in ("nw", "ne", "nq"):
            loads[name, i].wait()
    ze = [dot3(split(nw[i].T), split(ne[i])) for i in range(leaves - 1)]
    for i in range(leaves - 1):
        up_hi[i], up_lo[i] = split(dot3(split(ze[i]), split(nq[i])))
    for i in range(leaves):
        loads["rhs", i].wait()
        loads["lq", i].wait()
    ts = [dot3(split(rhs[i].T), split(lq[i]), NT) for i in range(leaves)]
    for i in range(leaves):
        loads["lw", i].wait()
        loads["le", i].wait()
    for i in range(leaves):
        values(i, ts[i])
    reduced = [dot3(split(ye[i, :R]), split(lw[i])) for i in range(leaves)]
    heights = {1: top(1)}
    k = 0
    while len(reduced) > 1:
        above = []
        for j in range(len(reduced) // 2):
            stacked[k] = cat(reduced[2 * j], reduced[2 * j + 1])
            above.append(dot3(split(stacked[k]), (up_hi[k], up_lo[k]), NT))
            k += 1
        reduced = above
    reduced = reduced[0]

    pl.semaphore_wait(barrier, len(messages))

    def exchange(index, a, d, src, dst):
        copy = pltpu.make_async_remote_copy(
            src_ref=src,
            dst_ref=dst,
            send_sem=send_sem.at[index],
            recv_sem=recv_sem.at[index],
            device_id={"leaf": me ^ (d << a)},
            device_id_type=MESH,
        )
        copy.start()
        return copy

    u_top = {}
    copies = {}
    index = 0
    current = reduced
    for number, (a, b) in enumerate(stages):
        first = number == 0
        moved = current
        for l in range(a, b):
            if l > a:
                moved = dot3(split(moved), mat(l, 0, 0, K), NT)
            if first:
                sent0[l] = moved.reshape(S, r, K)
            else:
                sent1[l] = moved
            for d in range(2 ** (l - a), 2 ** (l - a + 1)):
                if first and l + 1 < s:
                    copies[a, d] = exchange(index, a, d, sent0.at[l], full.at[d])
                elif first:
                    block = lax.rem(me ^ d, S)
                    copies[a, d] = exchange(index, a, d, sent0.at[l, block], part.at[index])
                else:
                    copies[a, d] = exchange(index, a, d, sent1.at[l], part.at[index])
                index += 1
        if first:
            for l in range(2, stages[1][1]):
                heights[l] = top(l)
        if number == 1:
            for l in range(stages[1][1], levels + 1):
                heights[l] = top(l)
            for k in range(leaves):
                solve(k)
            for k in range(leaves, 2 * leaves - 1):
                node(k)
            k = 2 * leaves - 2
            for l in range(1, s):
                ds = split(ud[k, R:])
                ud[k, :R] = ud[k, :R] - dot3(split(u_top[l]), ds)
                ud[k, R:] = -dot3(split(dn[l - 1, :K]), ds, TN)
            count_here, start = 1, k
            while count_here < leaves:
                kids = start - 2 * count_here
                for j in range(2 * count_here):
                    half = j % 2 * K
                    both = split(ud[start + j // 2, :, half : half + K])
                    shift = dot3(both, split(ud[kids + j, R:]))
                    ud[kids + j, :R] = ud[kids + j, :R] - shift[:R]
                    ud[kids + j, R:] = -shift[R:]
                start, count_here = kids, 2 * count_here
            for j in range(leaves):
                fin_hi[j], fin_lo[j] = split(ud[j, R:].T)
                out[j] = ud[j, :R].T
        if b == levels:
            m = None
            for l in range(levels - 1, s - 1, -1):
                lower = dn[l - 1, : heights[l] - K]
                step = mat(levels, 1, 0, K) if m is None else split(m)
                m = -dot3(split(lower), step)
            last = split(m)
        for l in range(a + 1, b + 1):
            group = range(2 ** (l - a - 1), 2 ** (l - a))
            if l == s:
                spread[...] = current.reshape(S, r, K)
                current = spread[pos]
            known = None
            if l < levels:
                h = heights[l]
                known = dot3(split(current), mat(l, 0, 0, h), NT)
            else:
                known = dot3(split(current), mat(l, 0, 0, K), NT)
                for low in range(levels - 1, s - 1, -1):
                    lower = split(dn[low - 1, : heights[low] - K])
                    known = u_top[low] - dot3(split(known), lower, NT)
            sib = None
            for d in group:
                copies[a, d].wait_recv()
                if first and l < s:
                    got = full[d].reshape(R, K)
                else:
                    got = part[messages.index((a, d))]
                sib = got if sib is None else sib + got
            if l < levels:
                both = known + dot3(split(sib), mat(l, 1, 0, h), NT)
                current = both[:, :K]
                u_top[l] = both[:, K:]
            else:
                answer = known + dot3(split(sib), last, NT)

    sendg[0] = answer[:, :K]
    sendg[1] = answer[:, K:]
    gcopies = []
    for d in range(S - 1, 0, -1):
        copy = pltpu.make_async_remote_copy(
            src_ref=sendg.at[1 if d >= S // 2 else 0],
            dst_ref=gath.at[pos],
            send_sem=gsend_sem.at[d],
            recv_sem=grecv_sem.at[d],
            device_id={"leaf": me ^ d},
            device_id_type=MESH,
        )
        copy.start()
        gcopies.append(copy)
    gath[pos] = answer[:, :K]
    for copy in gcopies:
        copy.wait_recv()
    g = split(gath[...].reshape(R, K))
    outs = []
    for j in range(leaves):
        out[j] = out[j] - dot3((fin_hi[j], fin_lo[j]), g, NT)
        copy = pltpu.make_async_copy(out.at[j], out_h.at[j], sem_out.at[j])
        copy.start()
        outs.append(copy)
    for copy in copies.values():
        copy.wait_send()
    for copy in gcopies:
        copy.wait_send()
    for copy in outs:
        copy.wait()


def body(n, *args):
    rhs, leaf_w, top_q = args[0], args[3], args[7]
    leaves, M, R = rhs.shape
    K = leaf_w.shape[2]
    levels = n.bit_length() - 1
    stages = plan(n)
    s = stages[0][1]
    S = 2**s
    r = R // S
    msgs = sum(2 ** (b - a) - 1 for a, b in stages)
    local = 2 * leaves - 1
    scratch = [pltpu.VMEM(x.shape, x.dtype) for x in args]
    scratch += [
        pltpu.VMEM((leaves, M, R), F32),
        pltpu.VMEM((local, R + K, M), F32),
        pltpu.VMEM((local, R + K, M), F32),
        pltpu.VMEM((leaves - 1, R, M), F32),
        pltpu.VMEM((leaves - 1, K, M), BF16),
        pltpu.VMEM((leaves - 1, K, M), BF16),
        pltpu.VMEM((s, S, r, K), F32),
        pltpu.VMEM((levels, r, K), F32),
        pltpu.VMEM((S, S, r, K), F32),
        pltpu.VMEM((msgs, r, K), F32),
        pltpu.VMEM((S, r, K), F32),
        pltpu.VMEM((2, r, K), F32),
        pltpu.VMEM((S, r, K), F32),
        pltpu.VMEM((levels, 2, 3 * K, K), BF16),
        pltpu.VMEM((levels, 2, 3 * K, K), BF16),
        pltpu.VMEM((levels, 2 * K, K), F32),
        pltpu.VMEM((leaves, M, K), BF16),
        pltpu.VMEM((leaves, M, K), BF16),
        pltpu.SemaphoreType.DMA((4 * leaves + 3 * (leaves - 1) + 3 * levels,)),
        pltpu.SemaphoreType.DMA((leaves,)),
        pltpu.SemaphoreType.DMA((msgs,)),
        pltpu.SemaphoreType.DMA((msgs,)),
        pltpu.SemaphoreType.DMA((S,)),
        pltpu.SemaphoreType.DMA((S,)),
    ]
    return pl.pallas_call(
        functools.partial(kernel, n),
        out_shape=jax.ShapeDtypeStruct((leaves, M, R), F32),
        in_specs=[pl.BlockSpec(memory_space=pl.ANY)] * len(args),
        out_specs=pl.BlockSpec(memory_space=pl.ANY),
        scratch_shapes=scratch,
        compiler_params=pltpu.CompilerParams(collective_id=0, has_side_effects=True),
    )(*args)


def solution(mesh):
    spec = P(("freq", "leaf"), None, None)
    return jax.shard_map(
        functools.partial(body, mesh.shape["leaf"]),
        mesh=mesh,
        in_specs=(spec,) * 10,
        out_specs=spec,
        check_vma=False,
    )
```

```python
import functools

import jax
import jax.numpy as jnp
from jax import lax
from jax.experimental import pallas as pl
from jax.experimental.pallas import tpu as pltpu
from jax.sharding import PartitionSpec as P

MESH = pl.DeviceIdType.MESH
F32, BF16 = jnp.float32, jnp.bfloat16
NN, NT, TN = ((1,), (0,)), ((1,), (1,)), ((0,), (0,))


def split(x):
    hi = x.astype(BF16)
    return hi, (x - hi.astype(F32)).astype(BF16)


def dot3(a, b, dims=NN):
    def one(x, y):
        return lax.dot_general(x, y, (dims, ((), ())), preferred_element_type=F32)

    return one(a[0], b[0]) + (one(a[0], b[1]) + one(a[1], b[0]))


def cat(*xs):
    return jnp.concatenate(xs, axis=1)


def plan(n):
    total = n.bit_length() - 1
    cuts = [0]
    while cuts[-1] < total:
        cuts.append(min(cuts[-1] + 2, total))
    if len(cuts) == 2:
        cuts = [0, total - 1, total]
    return list(zip(cuts[:-1], cuts[1:]))


def kernel(n, *refs):
    (rhs_h, lq_h, le_h, lw_h, nq_h, ne_h, nw_h, tq_h, te_h, tw_h, out, fin_hi, fin_lo, g_out,
     rhs, lq, le, lw, nq, ne, nw, tq, te, tw,
     ye, ud, stacked, up_hi, up_lo, sent0, sent1, full, part, spread, sendg, gath,
     mat_hi, mat_lo, dn,
     sem_in, send_sem, recv_sem, gsend_sem, grecv_sem) = refs
    stages = plan(n)
    levels = n.bit_length() - 1
    s = stages[0][1]
    S = 2**s
    leaves = rhs.shape[0]
    K = lw.shape[2]
    R = rhs.shape[2]
    r = R // S
    me = lax.axis_index("leaf")
    pos = lax.rem(me, S)

    def side(level):
        return lax.rem(me // 2 ** (level - 1), 2)

    loads = {}
    count = 0

    def load(name, src, dst, i):
        nonlocal count
        copy = pltpu.make_async_copy(src.at[i], dst.at[i], sem_in.at[count])
        copy.start()
        loads[name, i] = copy
        count += 1

    for i in range(leaves - 1):
        load("nw", nw_h, nw, i)
        load("ne", ne_h, ne, i)
        load("nq", nq_h, nq, i)
    for i in range(leaves):
        load("rhs", rhs_h, rhs, i)
        load("lq", lq_h, lq, i)
    for i in range(leaves):
        load("lw", lw_h, lw, i)
        load("le", le_h, le, i)
    for i in range(levels):
        load("tq", tq_h, tq, i)
        load("te", te_h, te, i)
        load("tw", tw_h, tw, i)

    messages = []
    for a, b in stages:
        for d in range(1, 2 ** (b - a)):
            messages.append((a, d))

    barrier = pltpu.get_barrier_semaphore()
    for a, d in messages:
        pl.semaphore_signal(
            barrier, inc=1, device_id={"leaf": me ^ (d << a)}, device_id_type=MESH
        )

    def factors(k):
        return (lq, le, lw, k) if k < leaves else (nq, ne, nw, k - leaves)

    def values(k, t):
        _, e, w, i = factors(k)
        ye[k] = dot3(split(jnp.concatenate([t, w[i].T], axis=0)), split(e[i]), NT)

    def solve(k):
        q, _, _, i = factors(k)
        ud[k] = dot3(split(ye[k]), split(q[i]))

    def node(k):
        i = k - leaves
        values(k, dot3(split(stacked[i]), split(nq[i]), NT))
        solve(k)

    def top(level):
        i = level - 1
        for name in ("tq", "te", "tw"):
            loads[name, i].wait()
        right = side(level) == 1
        q, w = tq[i], tw[i]
        if level == levels:
            rows = jnp.where(right, te[i, K:, :], te[i, :K, :])
            m = dot3(split(rows), split(q))
            height = K
        else:
            mine = jnp.where(right, q[:, K:], q[:, :K])
            z = cat(w, mine)
            if level == s:
                z = cat(z, jnp.where(right, q[:, :K], q[:, K:]))
            height = z.shape[1]
            ze = dot3(split(z), split(te[i]), TN)
            zs = split(ze)
            m = dot3(zs, split(q))
            dn[i, : height - K] = dot3(split(ze[K:]), split(w))
        own = jnp.where(right, m[:, K:], m[:, :K])
        sib = jnp.where(right, m[:, :K], m[:, K:])
        mat_hi[i, 0, :height], mat_lo[i, 0, :height] = split(own)
        mat_hi[i, 1, :height], mat_lo[i, 1, :height] = split(sib)
        return height

    def mat(level, which, low, high):
        i = level - 1
        return mat_hi[i, which, low:high], mat_lo[i, which, low:high]

    for i in range(leaves - 1):
        for name in ("nw", "ne", "nq"):
            loads[name, i].wait()
    ze = [dot3(split(nw[i].T), split(ne[i])) for i in range(leaves - 1)]
    for i in range(leaves - 1):
        up_hi[i], up_lo[i] = split(dot3(split(ze[i]), split(nq[i])))
    for i in range(leaves):
        loads["rhs", i].wait()
        loads["lq", i].wait()
    ts = [dot3(split(rhs[i].T), split(lq[i]), NT) for i in range(leaves)]
    for i in range(leaves):
        loads["lw", i].wait()
        loads["le", i].wait()
    for i in range(leaves):
        values(i, ts[i])
    reduced = [dot3(split(ye[i, :R]), split(lw[i])) for i in range(leaves)]
    heights = {1: top(1)}
    k = 0
    while len(reduced) > 1:
        above = []
        for j in range(len(reduced) // 2):
            stacked[k] = cat(reduced[2 * j], reduced[2 * j + 1])
            above.append(dot3(split(stacked[k]), (up_hi[k], up_lo[k]), NT))
            k += 1
        reduced = above
    reduced = reduced[0]

    pl.semaphore_wait(barrier, len(messages))

    def exchange(index, a, d, src, dst):
        copy = pltpu.make_async_remote_copy(
            src_ref=src,
            dst_ref=dst,
            send_sem=send_sem.at[index],
            recv_sem=recv_sem.at[index],
            device_id={"leaf": me ^ (d << a)},
            device_id_type=MESH,
        )
        copy.start()
        return copy

    u_top = {}
    copies = {}
    index = 0
    current = reduced
    for number, (a, b) in enumerate(stages):
        first = number == 0
        moved = current
        for l in range(a, b):
            if l > a:
                moved = dot3(split(moved), mat(l, 0, 0, K), NT)
            if first:
                sent0[l] = moved.reshape(S, r, K)
            else:
                sent1[l] = moved
            for d in range(2 ** (l - a), 2 ** (l - a + 1)):
                if first and l + 1 < s:
                    copies[a, d] = exchange(index, a, d, sent0.at[l], full.at[d])
                elif first:
                    block = lax.rem(me ^ d, S)
                    copies[a, d] = exchange(index, a, d, sent0.at[l, block], part.at[index])
                else:
                    copies[a, d] = exchange(index, a, d, sent1.at[l], part.at[index])
                index += 1
        if first:
            for l in range(2, stages[1][1]):
                heights[l] = top(l)
        if number == 1:
            for l in range(stages[1][1], levels + 1):
                heights[l] = top(l)
            for k in range(leaves):
                solve(k)
            for k in range(leaves, 2 * leaves - 1):
                node(k)
            k = 2 * leaves - 2
            for l in range(1, s):
                ds = split(ud[k, R:])
                ud[k, :R] = ud[k, :R] - dot3(split(u_top[l]), ds)
                ud[k, R:] = -dot3(split(dn[l - 1, :K]), ds, TN)
            count_here, start = 1, k
            while count_here < leaves:
                kids = start - 2 * count_here
                for j in range(2 * count_here):
                    half = j % 2 * K
                    both = split(ud[start + j // 2, :, half : half + K])
                    shift = dot3(both, split(ud[kids + j, R:]))
                    ud[kids + j, :R] = ud[kids + j, :R] - shift[:R]
                    ud[kids + j, R:] = -shift[R:]
                start, count_here = kids, 2 * count_here
            for j in range(leaves):
                fin_hi[j], fin_lo[j] = split(ud[j, R:].T)
                out[j] = ud[j, :R].T
        if b == levels:
            m = None
            for l in range(levels - 1, s - 1, -1):
                lower = dn[l - 1, : heights[l] - K]
                step = mat(levels, 1, 0, K) if m is None else split(m)
                m = -dot3(split(lower), step)
            last = split(m)
        for l in range(a + 1, b + 1):
            group = range(2 ** (l - a - 1), 2 ** (l - a))
            if l == s:
                spread[...] = current.reshape(S, r, K)
                current = spread[pos]
            known = None
            if l < levels:
                h = heights[l]
                known = dot3(split(current), mat(l, 0, 0, h), NT)
            else:
                known = dot3(split(current), mat(l, 0, 0, K), NT)
                for low in range(levels - 1, s - 1, -1):
                    lower = split(dn[low - 1, : heights[low] - K])
                    known = u_top[low] - dot3(split(known), lower, NT)
            sib = None
            for d in group:
                copies[a, d].wait_recv()
                if first and l < s:
                    got = full[d].reshape(R, K)
                else:
                    got = part[messages.index((a, d))]
                sib = got if sib is None else sib + got
            if l < levels:
                both = known + dot3(split(sib), mat(l, 1, 0, h), NT)
                current = both[:, :K]
                u_top[l] = both[:, K:]
            else:
                answer = known + dot3(split(sib), last, NT)

    sendg[0] = answer[:, :K]
    sendg[1] = answer[:, K:]
    gcopies = []
    for d in range(S - 1, 0, -1):
        copy = pltpu.make_async_remote_copy(
            src_ref=sendg.at[1 if d >= S // 2 else 0],
            dst_ref=gath.at[pos],
            send_sem=gsend_sem.at[d],
            recv_sem=grecv_sem.at[d],
            device_id={"leaf": me ^ d},
            device_id_type=MESH,
        )
        copy.start()
        gcopies.append(copy)
    gath[pos] = answer[:, :K]
    for copy in gcopies:
        copy.wait_recv()
    g_out[...] = gath[...].reshape(R, K)
    for copy in copies.values():
        copy.wait_send()
    for copy in gcopies:
        copy.wait_send()


def finish(base, fin_hi, fin_lo, g_in, out_h, out, sem):
    g = split(g_in[...])
    copies = []
    for j in range(base.shape[0]):
        out[j] = base[j] - dot3((fin_hi[j], fin_lo[j]), g, NT)
        copies.append(pltpu.make_async_copy(out.at[j], out_h.at[j], sem.at[j]))
        copies[-1].start()
    for copy in copies:
        copy.wait()


def body(n, *args):
    rhs, leaf_w, top_q = args[0], args[3], args[7]
    leaves, M, R = rhs.shape
    K = leaf_w.shape[2]
    levels = n.bit_length() - 1
    stages = plan(n)
    s = stages[0][1]
    S = 2**s
    r = R // S
    msgs = sum(2 ** (b - a) - 1 for a, b in stages)
    local = 2 * leaves - 1
    scratch = [pltpu.VMEM(x.shape, x.dtype) for x in args]
    scratch += [
        pltpu.VMEM((local, R + K, M), F32),
        pltpu.VMEM((local, R + K, M), F32),
        pltpu.VMEM((leaves - 1, R, M), F32),
        pltpu.VMEM((leaves - 1, K, M), BF16),
        pltpu.VMEM((leaves - 1, K, M), BF16),
        pltpu.VMEM((s, S, r, K), F32),
        pltpu.VMEM((levels, r, K), F32),
        pltpu.VMEM((S, S, r, K), F32),
        pltpu.VMEM((msgs, r, K), F32),
        pltpu.VMEM((S, r, K), F32),
        pltpu.VMEM((2, r, K), F32),
        pltpu.VMEM((S, r, K), F32),
        pltpu.VMEM((levels, 2, 3 * K, K), BF16),
        pltpu.VMEM((levels, 2, 3 * K, K), BF16),
        pltpu.VMEM((levels, 2 * K, K), F32),
        pltpu.SemaphoreType.DMA((4 * leaves + 3 * (leaves - 1) + 3 * levels,)),
        pltpu.SemaphoreType.DMA((msgs,)),
        pltpu.SemaphoreType.DMA((msgs,)),
        pltpu.SemaphoreType.DMA((S,)),
        pltpu.SemaphoreType.DMA((S,)),
    ]
    vmem = pl.BlockSpec(memory_space=pltpu.VMEM)
    anywhere = pl.BlockSpec(memory_space=pl.ANY)
    parts = pl.pallas_call(
        functools.partial(kernel, n),
        out_shape=(
            pltpu.VMEM((leaves, M, R), F32),
            pltpu.VMEM((leaves, M, K), BF16),
            pltpu.VMEM((leaves, M, K), BF16),
            pltpu.VMEM((R, K), F32),
        ),
        in_specs=[anywhere] * len(args),
        out_specs=(vmem,) * 4,
        scratch_shapes=scratch,
        compiler_params=pltpu.CompilerParams(
            collective_id=0, has_side_effects=True
        ),
    )(*args)
    return pl.pallas_call(
        finish,
        out_shape=jax.ShapeDtypeStruct((leaves, M, R), F32),
        in_specs=[vmem] * 4,
        out_specs=anywhere,
        scratch_shapes=[
            pltpu.VMEM((leaves, M, R), F32),
            pltpu.SemaphoreType.DMA((leaves,)),
        ],
        compiler_params=pltpu.CompilerParams(vmem_limit_bytes=8 * 2**20),
    )(*parts)


def solution(mesh):
    spec = P(("freq", "leaf"), None, None)
    return jax.shard_map(
        functools.partial(body, mesh.shape["leaf"]),
        mesh=mesh,
        in_specs=(spec,) * 10,
        out_specs=spec,
        check_vma=False,
    )
```
